512 devices in a mesh: row: 32 (over y_lo, z), col: 16 (over x, y_hi, core).
Axes of the slice: x: 4, y: 8 (y_hi: 2, y_lo: 4; y = y_hi * 4 + y_lo), z: 8, core: 2. Of those that a mesh axis runs over, the one named last changes fastest.
Arguments:
- acts: bfloat16 [4096, 12288], P('row', 'col'), may hold values from -6 to 6
- grads: bfloat16 [4096, 12288], P('col', 'row'), may hold values from -0.19921875 to 0.19921875
- next_acts: bfloat16 [1024, 12288], P('row', 'col'), may hold values from -6 to 6
- weight: bfloat16 [12288, 12288], P('row', 'col'), may hold values from -0.0546875 to 0.0546875
- moment: float32 [12288, 12288], P('row', 'col'), may hold values from -6 to 6
- second: float32 [12288, 12288], P('row', 'col'), may hold values from 0.05 to 5
- left_bank: bfloat16 [4, 384, 384], replicated, may hold values from -1 to 1, as said below
- right_bank: bfloat16 [4, 768, 768], P(None, 'row'), may hold values from -1 to 1, as said below
- left_index: int32 [32, 16], P('row', 'col'), may hold values from 0 to 3
- right_index: int32 [32, 16], P('row', 'col'), may hold values from 0 to 3
Outputs:
- update: bfloat16 [12288, 12288], P('row', 'col')
- next_out: bfloat16 [1024, 12288], P('col', 'row')
The draws below stay inside these ranges and needn't reach their ends.
Inputs may be any that keep to these rules, and one draw needn't show every extreme that they name: `left_bank`: each basis is an orthogonal matrix rounded to bfloat16. `right_bank`: each basis is an orthogonal matrix rounded to bfloat16.
All inputs are finite; a program needn't handle non-finite values.
Results may differ from the reference program's by a relative error of at most 0.008.
Values may be sent and summed in bfloat16 or wider, within the bound.
No kernel may reach another device: no remote copies, remote signals or barrier semaphores. Data moves between devices by JAX's collectives and lax.ppermute only.
A program may use at most 64 MiB of HBM per device.

```python
import math
import jax
import jax.numpy as jnp
from jax import lax

BO = 384
BI = 768
BANK = 4
TOKENS = 4096
NEXT = 1024
D_OUT = 12288
D_IN = 12288
N_ROW = 32
N_COL = 16


def orthogonal_bank(key, count, order):
    normals = jax.random.normal(key, (count, order, order), jnp.float32)
    factors = jax.vmap(lambda matrix: jnp.linalg.qr(matrix)[0])(normals)
    return factors.astype(jnp.bfloat16)


def draw_left_bank(key, part):
    return orthogonal_bank(jax.random.fold_in(key, 11), BANK, BO)


def draw_right_bank(key, part):
    return orthogonal_bank(jax.random.fold_in(key, 23), BANK, BI)


def plant(values, stream_key, least, top_value):
    longest = values.shape.index(max(values.shape))
    spots = []
    for shift in (0, 1):
        where = [jax.random.randint(jax.random.fold_in(stream_key, axis), (), 0, length) for axis, length in enumerate(values.shape)]
        where[longest] = (where[longest] + shift) % values.shape[longest]
        spots.append(tuple(where))
    return values.at[spots[0]].set(least).at[spots[1]].set(top_value)


def block_scale(key, dims, split, least, top_value):
    loudness, own = 1.0, jax.random.fold_in(key, 6)
    for axis_at, shards_of in split:
        draws = jnp.exp(jax.random.uniform(jax.random.fold_in(own, axis_at), (shards_of,), jnp.float32, least / len(split), top_value / len(split)))
        loudness = loudness * jnp.repeat(draws, dims[axis_at] // shards_of).reshape([-1 if axis == axis_at else 1 for axis in range(len(dims))])
    return loudness


def normal_values(rng, extent, deviation, reach, cuts=(), dtype=jnp.bfloat16):
    drawn = jax.random.normal(rng, extent, jnp.float32) * deviation
    if len(cuts) > 0:
        drawn = block_scale(rng, extent, cuts, -0.22, 0.18) * drawn
    return jnp.clip(drawn, min=-reach, max=reach).astype(dtype)


def setup_inputs(seed: int = 0) -> dict:
    streams_of = jax.random.split(jax.random.key(seed), 11)
    return {
        "acts": normal_values(streams_of[0], (TOKENS, D_IN), 1.0, 6.0, ((0, 32), (1, 16))),
        "grads": normal_values(streams_of[1], (TOKENS, D_OUT), 0.03, 0.19921875, ((0, 16), (1, 32))),
        "next_acts": normal_values(streams_of[2], (NEXT, D_IN), 1.0, 6.0, ((0, 32), (1, 16))),
        "weight": normal_values(streams_of[3], (D_OUT, D_IN), D_IN ** -0.5, 0.0546875, ((0, 32), (1, 16))),
        "moment": normal_values(streams_of[4], (D_OUT, D_IN), 1.0, 6.0, ((0, 32), (1, 16)), jnp.float32),
        "second": jnp.clip(jnp.exp(math.log(5.0) - 4.6051702 * jax.random.uniform(streams_of[5], (D_OUT, D_IN), jnp.float32) ** block_scale(streams_of[5], (D_OUT, D_IN), ((0, 32), (1, 16)), -0.2, 0.2)), 0.05, 5.0),
        "left_bank": draw_left_bank(jax.random.fold_in(streams_of[10], 71), 0),
        "right_bank": draw_right_bank(jax.random.fold_in(streams_of[10], 71), 0),
        "left_index": plant(jax.random.randint(streams_of[8], (N_ROW, N_COL), 0, BANK), jax.random.fold_in(streams_of[8], 1), 0, BANK - 1).astype(jnp.int32),
        "right_index": plant(jax.random.randint(streams_of[9], (N_ROW, N_COL), 0, BANK), jax.random.fold_in(streams_of[9], 1), 0, BANK - 1).astype(jnp.int32),
    }


HIGH = lax.Precision.HIGHEST

def to_blocks(array):
    return array.reshape(N_ROW, BO, N_COL, BI).transpose(0, 2, 1, 3).reshape(N_ROW * N_COL, BO, BI)

def from_blocks(array):
    return array.reshape(N_ROW, N_COL, BO, BI).transpose(0, 2, 1, 3).reshape(N_ROW * BO, N_COL * BI)

def reference(acts, grads, next_acts, weight, moment, second, left_bank, right_bank, left_index, right_index):
    f32 = jnp.float32
    gradient = jnp.dot(grads.astype(f32).T, acts.astype(f32), precision=HIGH).astype(jnp.bfloat16)

    def one_block(items):
        grad_block, weight_block, moment_block, second_block, left_pick, right_pick = items
        left_basis = lax.dynamic_index_in_dim(left_bank, left_pick, 0, keepdims=False).astype(f32)
        right_basis = lax.dynamic_index_in_dim(right_bank, right_pick, 0, keepdims=False).astype(f32)
        half = jnp.dot(left_basis.T, grad_block.astype(f32), precision=HIGH).astype(jnp.bfloat16)
        rotated = jnp.dot(half.astype(f32), right_basis, precision=HIGH)
        new_moment = 0.8 * moment_block + 0.2 * rotated
        new_second = 0.9 * second_block + 0.1 * rotated * rotated
        scaled = (new_moment / (jnp.sqrt(new_second) + 1e-08)).astype(jnp.bfloat16)
        back = jnp.dot(left_basis, scaled.astype(f32), precision=HIGH).astype(jnp.bfloat16)
        update_full = jnp.dot(back.astype(f32), right_basis.T, precision=HIGH)
        new_weight = (weight_block.astype(f32) - 0.001 * update_full).astype(jnp.bfloat16)
        return (update_full.astype(jnp.bfloat16), new_weight)
    updates, weights = lax.map(one_block, (to_blocks(gradient), to_blocks(weight), to_blocks(moment), to_blocks(second), left_index.reshape(-1).astype(jnp.int32), right_index.reshape(-1).astype(jnp.int32)))
    update = from_blocks(updates)
    new_weight = from_blocks(weights)
    next_out = jnp.dot(next_acts.astype(f32), new_weight.astype(f32).T, precision=HIGH).astype(jnp.bfloat16)
    return (update, next_out)
```

```python
import jax
import jax.numpy as jnp
from jax import lax
from jax.sharding import Mesh
from jax.sharding import PartitionSpec as P

ROW = ("yl", "z")
COL = ("x", "yh", "c")
BF = jnp.bfloat16
F32 = jnp.float32
U32 = jnp.uint32


def ring(n, shift):
    return [(i, (i + shift) % n) for i in range(n)]


def xor(n, mask):
    return [(i, i ^ mask) for i in range(n)]


def place(buffer, piece, where):
    return lax.dynamic_update_slice(
        buffer, piece[None], (where,) + (jnp.uint32(0),) * piece.ndim
    )


def per_device(
    acts, grads, next_acts, weight, moment, second, left_bank, right_bank, left_index, right_index
):
    yl, z, x, yh, c = (lax.axis_index(a).astype(U32) for a in ("yl", "z", "x", "yh", "c"))
    zero = jnp.uint32(0)

    own = jnp.concatenate([acts, next_acts], axis=0)
    from1 = lax.ppermute(own, "yl", xor(4, 1))
    grads_far = lax.ppermute(grads, "yh", ring(2, 1))
    from2 = lax.ppermute(own, "yl", xor(4, 2))
    from3 = lax.ppermute(own, "yl", xor(4, 3))

    picks = jnp.broadcast_to(right_index[None], (32, 1, 1))
    picks = lax.all_to_all(picks, ROW, split_axis=0, concat_axis=0, tiled=True)
    outgoing = jnp.take(right_bank, picks.reshape(32), axis=0)
    incoming = lax.all_to_all(outgoing, ROW, split_axis=0, concat_axis=0, tiled=True)
    right_basis = incoming.reshape(768, 768)

    left_basis = lax.dynamic_index_in_dim(left_bank, left_index[0, 0], 0, keepdims=False)

    pair = jnp.zeros((2, 256, 384), BF)
    pair = place(place(pair, grads, yh), grads_far, 1 - yh)
    by_x = [pair] + [lax.ppermute(pair, "x", ring(4, s)) for s in (1, 3, 2)]
    mine = jnp.zeros((4, 2, 256, 384), BF)
    for s, piece in zip((0, 1, 3, 2), by_x):
        mine = place(mine, piece, yl ^ ((x - jnp.uint32(s)) & 3))
    theirs = lax.ppermute(mine, "c", ring(2, 1))
    both = jnp.zeros((2, 4, 2, 256, 384), BF)
    both = place(place(both, mine, c), theirs, 1 - c)
    both = both.reshape(2, 4, 2, 2, 128, 384)

    streams = (jnp.stack([own, from1]), jnp.stack([from2, from3]))
    blocks = [{0: streams[0]}, {0: streams[1]}]
    reach = ((4, 3), (3, 4))
    for step in (1, 2, 3, 4):
        for k in (0, 1):
            if step <= reach[k][0]:
                blocks[k][step] = lax.ppermute(blocks[k][step - 1], "z", ring(8, 1))
            if step <= reach[k][1]:
                blocks[k][-step] = lax.ppermute(blocks[k][1 - step], "z", ring(8, 7))

    total = None
    order = [0, 1, -1, 2, -2, 3, -3]
    for s in order + [4]:
        for k in (0, 1):
            if s == 4 and k == 1:
                key = -4
            else:
                key = s
            src = (z - jnp.uint32(key % 8)) & 7
            g = lax.dynamic_slice(
                both,
                ((src >> 1) & 1, jnp.uint32(2 * k), src >> 2, src & 1, zero, zero),
                (1, 2, 1, 1, 128, 384),
            ).reshape(2, 128, 384)
            part = lax.dot_general(
                g,
                blocks[k][key][:, :128],
                (((0, 1), (0, 1)), ((), ())),
                preferred_element_type=F32,
            )
            total = part if total is None else total + part
    gradient = total.astype(BF)

    half = lax.dot_general(
        left_basis, gradient, (((0,), (0,)), ((), ())), preferred_element_type=F32
    ).astype(BF)
    rotated = jnp.dot(half, right_basis, preferred_element_type=F32)
    new_moment = 0.8 * moment + 0.2 * rotated
    new_second = 0.9 * second + 0.1 * rotated * rotated
    scaled = (new_moment / (jnp.sqrt(new_second) + 1e-08)).astype(BF)
    back_left = jnp.dot(left_basis, scaled, preferred_element_type=F32).astype(BF)
    update_full = lax.dot_general(
        back_left, right_basis, (((1,), (1,)), ((), ())), preferred_element_type=F32
    )
    new_weight = (weight.astype(F32) - 0.001 * update_full).astype(BF)

    rows = []
    for s in (0, 1, 2, 3, 4, -3, -2, -1):
        for k in (0, 1):
            key = -4 if (s == 4 and k == 1) else s
            rows.append(blocks[k][key][:, 128:].reshape(64, 768))
    full_next = jnp.concatenate(rows, axis=0)
    summed = lax.dot_general(
        full_next, new_weight, (((1,), (1,)), ((), ())), preferred_element_type=F32
    ).reshape(32, 32, 384)
    xs = jnp.arange(4, dtype=U32)[:, None, None]
    yhs = jnp.arange(2, dtype=U32)[None, :, None]
    hs = jnp.arange(2, dtype=U32)[None, None, :]

    def rows_of(core):
        src = 4 * yhs + 2 * core + hs
        return (((z - src) & 7) * 4 + (yl ^ xs)).reshape(16)

    away = jnp.take(summed, rows_of(1 - c), axis=0).astype(BF)
    keep = jnp.take(summed, rows_of(c), axis=0)
    keep = keep + lax.ppermute(away, "c", ring(2, 1)).astype(F32)
    keep = keep.astype(BF).reshape(8, 64, 384)
    arrived = lax.all_to_all(keep, ("x", "yh"), split_axis=0, concat_axis=0, tiled=True)
    next_out = arrived.astype(F32).sum(axis=0).astype(BF)
    return update_full.astype(BF), next_out


def solution(mesh):
    finer = Mesh(mesh.devices.reshape(4, 8, 4, 2, 2), ("yl", "z", "x", "yh", "c"))
    in_specs = (
        P(ROW, COL),
        P(COL, ROW),
        P(ROW, COL),
        P(ROW, COL),
        P(ROW, COL),
        P(ROW, COL),
        P(),
        P(None, ROW, None),
        P(ROW, COL),
        P(ROW, COL),
    )
    out_specs = (P(ROW, COL), P(COL, ROW))
    return jax.shard_map(
        per_device, mesh=finer, in_specs=in_specs, out_specs=out_specs, check_vma=False
    )
```

```python
import functools

import jax
import jax.numpy as jnp
from jax import lax
from jax.experimental import pallas as pl
from jax.experimental.pallas import tpu as pltpu
from jax.sharding import Mesh
from jax.sharding import PartitionSpec as P


ROW = ("yl", "z")
COL = ("x", "yh", "c")
BF = jnp.bfloat16
F32 = jnp.float32


ACTS, NEXT, BANK = 128, 32, 48
ROWS = ACTS + NEXT + BANK

YL, Z, YH, C, LEFT, MY_B, MY_HAS, THEIR_B = range(8)

TT = (((0,), (0,)), ((), ()))
NT = (((1,), (1,)), ((), ()))
NN = (((1,), (0,)), ((), ()))


def dot(a, b, dims):
    return lax.dot_general(a, b, dims, preferred_element_type=F32)


def ring(n, shift):
    return [(i, (i + shift) % n) for i in range(n)]


def xor(n, mask):
    return [(i, i ^ mask) for i in range(n)]


def call(kernel, outs, flops, *args, aliases={}):
    vmem = pl.BlockSpec(memory_space=pltpu.VMEM)
    smem = pl.BlockSpec(memory_space=pltpu.SMEM)
    shapes = [jax.ShapeDtypeStruct(s, d) for s, d in outs]
    nbytes = sum(a.size * a.dtype.itemsize for a in args[1:])
    return pl.pallas_call(
        kernel,
        out_shape=shapes,
        in_specs=[smem] + [vmem] * (len(args) - 1),
        out_specs=[vmem] * len(shapes),
        compiler_params=pltpu.CompilerParams(vmem_limit_bytes=20 * 1024 * 1024),
        cost_estimate=pl.CostEstimate(flops=flops, bytes_accessed=nbytes, transcendentals=0),
        input_output_aliases=aliases,
    )(*args)


def source(sc, m, step, e):
    shift = m >> 1
    w = (sc[Z] + shift) & 7
    k, par = w >> 1, w & 1
    pair = {1: k, 2: k - 1 + 2 * par, 3: k + 1 - 2 * par, 4: k + 2}[step]
    return (2 * (pair & 3) + (par ^ ((step - 1) & 1) ^ e) - shift) & 7


def chunk_sum(key, sc, mine, theirs, block):
    m, step = key
    parts = []
    for e in (0, 1):
        src = source(sc, m, step, e)
        far_core = (((src >> 1) & 1) ^ sc[C]) == 1
        dyh = (src >> 2) ^ sc[YH]
        h = src & 1
        near = mine[m >> 1, m & 1, dyh, h]
        far = theirs[m >> 1, m & 1, dyh, h]
        parts.append(jnp.where(far_core, far, near))
    g = jnp.concatenate(parts, axis=0)
    return dot(g, block[:, :ACTS].reshape(2 * ACTS, 768), TT)


def first_kernel(keys, sc, mine, theirs, *refs):
    blocks, out = refs[:-1], refs[-1]
    for i, (key, block) in enumerate(zip(keys, blocks)):
        part = chunk_sum(key, sc, mine, theirs, block)
        if i == 0:
            out[...] = part
        else:
            out[...] += part


def next_kernel(keys, sc, mine, theirs, acc, *refs):
    blocks, out = refs[:-1], refs[-1]
    for i, (key, block) in enumerate(zip(keys, blocks)):
        part = chunk_sum(key, sc, mine, theirs, block)
        if i == 0:
            out[...] = acc[...] + part
        else:
            out[...] += part


def last_kernel(keys, sc, mine, theirs, acc, left, *refs):
    blocks, out = refs[:-1], refs[-1]
    total = acc[...]
    for key, block in zip(keys, blocks):
        total = total + chunk_sum(key, sc, mine, theirs, block)
    out[...] = dot(left[sc[LEFT]], total.astype(BF), TT).astype(BF)


def sort_kernel(keys, sc, *refs):
    blocks, (tokens, own, send) = refs[: len(keys)], refs[-3:]
    for (m, step), block in zip(keys, blocks):
        peer = sc[YL] ^ m
        for e in (0, 1):
            src = source(sc, m, step, e)
            dc = ((src >> 1) & 1) ^ sc[C]
            tokens[dc, peer, src >> 2, src & 1] = block[e, ACTS : ACTS + NEXT]
            even = block[e, ACTS + NEXT : ACTS + NEXT + 24]
            odd = block[e, ACTS + NEXT + 24 : ROWS]
            own[peer, src] = jnp.where(sc[MY_B] == 1, odd, even)
            send[peer, src] = jnp.where(sc[THEIR_B] == 1, odd, even)


def update_kernel(sc, half, own, got, moment, second, weight, left, tokens, update, fresh, away, right, back):
    right[...] = jnp.where(sc[MY_HAS] == 1, own[...], got[...])
    basis = left[sc[LEFT]]
    for n in range(3):
        cols = slice(256 * n, 256 * n + 256)
        rotated = dot(half[...], right[:, cols], NN)
        new_moment = 0.8 * moment[:, cols] + 0.2 * rotated
        new_second = 0.9 * second[:, cols] + 0.1 * rotated * rotated
        scaled = (new_moment / (jnp.sqrt(new_second) + 1e-08)).astype(BF)
        back[:, cols] = dot(basis, scaled, NN).astype(BF)
    for n in range(3):
        cols = slice(256 * n, 256 * n + 256)
        full = dot(back[...], right[cols, :], NT)
        update[:, cols] = full.astype(BF)
        fresh[:, cols] = (weight[:, cols].astype(F32) - 0.001 * full).astype(BF)
    away[...] = dot(tokens[1], fresh[...], NT).astype(BF)


def keep_kernel(sc, tokens, fresh, keep):
    keep[...] = dot(tokens[0], fresh[...], NT)


def two(near, far, first):
    spots = lax.broadcasted_iota(jnp.int32, (2,) + (1,) * near.ndim, 0)
    return lax.optimization_barrier(jnp.where(spots == first, near[None], far[None]))


def per_device(
    acts, grads, next_acts, weight, moment, second, left_bank, right_bank, left_index, right_index
):
    yl, z, x, yh, c = (lax.axis_index(a) for a in ("yl", "z", "x", "yh", "c"))

    bank_half = lax.dynamic_slice(
        right_bank, (c.astype(jnp.uint32) * 2, jnp.uint32(0), jnp.uint32(0)), (2, 24, 768)
    )
    own = jnp.concatenate([acts, next_acts, bank_half.reshape(BANK, 768)], axis=0)
    grads_far = lax.ppermute(grads, "yh", ring(2, 1))
    starts = [own] + [lax.ppermute(own, "yl", xor(4, m)) for m in (1, 2, 3)]

    right_own = right_index[0, 0]
    right_far = lax.ppermute(right_index, "c", ring(2, 1))[0, 0]
    values = (
        yl, z, yh, c, left_index[0, 0],
        right_own & 1, ((right_own >> 1) == c).astype(jnp.int32), right_far & 1,
    )
    spots = jnp.arange(len(values), dtype=jnp.int32)
    sc = sum(jnp.where(spots == i, v, 0) for i, v in enumerate(values))

    apart = x ^ yl
    pair = two(grads, grads_far, 0)
    pair_far = lax.ppermute(pair, "x", xor(4, 1))
    quad = two(pair, pair_far, apart & 1)
    quad_far = lax.ppermute(quad, "x", xor(4, 3))
    mine = two(quad, quad_far, apart >> 1)
    theirs = lax.ppermute(mine, "c", ring(2, 1))
    mine = mine.reshape(2, 2, 2, 2, 128, 384)
    theirs = theirs.reshape(2, 2, 2, 2, 128, 384)

    even = xor(8, 1)
    odd = [(i, (i + 1) % 8 if i % 2 else (i - 1) % 8) for i in range(8)]
    blocks = {}
    for m in range(4):
        links = (even, odd) if m < 2 else (odd, even)
        got = lax.ppermute(starts[m], "z", links[0])
        blocks[m, 1] = lax.optimization_barrier(jnp.stack([starts[m], got]))
        for step in (2, 3, 4):
            blocks[m, step] = lax.ppermute(blocks[m, step - 1], "z", links[(step - 1) % 2])

    def of(*keys):
        return keys, [blocks[k] for k in keys]

    acc_shape = [((384, 768), F32)]
    chunk_flops = 2 * 256 * 384 * 768
    late_keys = ((2, 4), (3, 4))
    groups = (
        [(m, 1) for m in range(4)],
        [(m, 2) for m in range(4)],
        [(m, 3) for m in range(4)] + [(0, 4), (1, 4)],
    )
    acc = ()
    for i, group in enumerate(groups):
        keys, held = of(*group)
        acc = call(
            functools.partial(next_kernel if i else first_kernel, keys),
            acc_shape, len(keys) * chunk_flops, sc, mine, theirs, *acc, *held,
        )
    (acc,) = acc
    sorted_shapes = [((2, 4, 2, 2, NEXT, 768), BF), ((4, 8, 24, 768), BF), ((4, 8, 24, 768), BF)]
    keys, held = of(*(k for group in groups for k in group))
    early = call(functools.partial(sort_kernel, keys), sorted_shapes, 2 * chunk_flops, sc, *held)
    keys, held = of(*late_keys)
    tokens, right_mine, right_send = call(
        functools.partial(sort_kernel, keys), sorted_shapes, chunk_flops, sc, *held, *early,
        aliases={3: 0, 4: 1, 5: 2},
    )
    right_got = lax.ppermute(right_send, "c", ring(2, 1))
    keys, held = of(*late_keys)
    (half,) = call(
        functools.partial(last_kernel, keys),
        [((384, 768), BF)], 4 * chunk_flops, sc, mine, theirs, acc, left_bank, *held,
    )
    tokens = tokens.reshape(2, 512, 768)
    update, fresh, away = pl.pallas_call(
        update_kernel,
        out_shape=[
            jax.ShapeDtypeStruct((384, 768), BF),
            jax.ShapeDtypeStruct((384, 768), BF),
            jax.ShapeDtypeStruct((512, 384), BF),
        ],
        in_specs=[pl.BlockSpec(memory_space=pltpu.SMEM)] + [pl.BlockSpec(memory_space=pltpu.VMEM)] * 8,
        out_specs=[pl.BlockSpec(memory_space=pltpu.VMEM)] * 3,
        scratch_shapes=[pltpu.VMEM((768, 768), BF), pltpu.VMEM((384, 768), BF)],
        compiler_params=pltpu.CompilerParams(vmem_limit_bytes=20 * 1024 * 1024),
        cost_estimate=pl.CostEstimate(flops=2 * 10**9, bytes_accessed=10**7, transcendentals=0),
        name="update",
    )(
        sc, half, right_mine.reshape(768, 768), right_got.reshape(768, 768),
        moment, second, weight, left_bank, tokens,
    )
    away_got = lax.ppermute(away, "c", ring(2, 1))
    (keep,) = call(keep_kernel, [((512, 384), F32)], 3 * 10**8, sc, tokens, fresh)
    keep = (keep + away_got.astype(F32)).astype(BF).reshape(8, 64, 384)
    arrived = lax.all_to_all(keep, ("x", "yh"), split_axis=0, concat_axis=0, tiled=True)
    next_out = arrived.astype(F32).sum(axis=0).astype(BF)
    return update, next_out


def solution(mesh):
    finer = Mesh(mesh.devices.reshape(4, 8, 4, 2, 2), ("yl", "z", "x", "yh", "c"))
    in_specs = (
        P(ROW, COL),
        P(COL, ROW),
        P(ROW, COL),
        P(ROW, COL),
        P(ROW, COL),
        P(ROW, COL),
        P(),
        P(None, ROW, None),
        P(ROW, COL),
        P(ROW, COL),
    )
    out_specs = (P(ROW, COL), P(COL, ROW))

    return jax.shard_map(
        per_device, mesh=finer, in_specs=in_specs, out_specs=out_specs, check_vma=False
    )
```

```python
import functools

import jax
import jax.numpy as jnp
from jax import lax
from jax.experimental import pallas as pl
from jax.experimental.pallas import tpu as pltpu
from jax.sharding import Mesh
from jax.sharding import PartitionSpec as P


ROW = ("yl", "z")
COL = ("x", "yh", "c")
BF = jnp.bfloat16
F32 = jnp.float32


ACTS, NEXT, BANK = 128, 32, 48
ROWS = NEXT + BANK

YL, Z, YH, C, LEFT, MY_B, MY_HAS, THEIR_B = range(8)

TT = (((0,), (0,)), ((), ()))
NT = (((1,), (1,)), ((), ()))
NN = (((1,), (0,)), ((), ()))


def dot(a, b, dims):
    return lax.dot_general(a, b, dims, preferred_element_type=F32)


def stack_of(*parts):
    return lax.optimization_barrier(jnp.stack(parts))


def ring(n, shift):
    return [(i, (i + shift) % n) for i in range(n)]


def xor(n, mask):
    return [(i, i ^ mask) for i in range(n)]


def call(kernel, outs, flops, *args, aliases={}):
    vmem = pl.BlockSpec(memory_space=pltpu.VMEM)
    smem = pl.BlockSpec(memory_space=pltpu.SMEM)
    shapes = [jax.ShapeDtypeStruct(s, d) for s, d in outs]
    nbytes = sum(a.size * a.dtype.itemsize for a in args[1:])
    return pl.pallas_call(
        kernel,
        out_shape=shapes,
        in_specs=[smem] + [vmem] * (len(args) - 1),
        out_specs=[vmem] * len(shapes),
        compiler_params=pltpu.CompilerParams(vmem_limit_bytes=24 * 1024 * 1024),
        cost_estimate=pl.CostEstimate(flops=flops, bytes_accessed=nbytes, transcendentals=0),
        input_output_aliases=aliases,
    )(*args)


def chunk_grads(step, f, sc, mine, theirs):
    src = (sc[Z] - step) & 7
    far_core = (((src >> 1) & 1) ^ sc[C]) == 1
    dyh = (src >> 2) ^ sc[YH]
    h = src & 1
    near = mine[:, f, dyh, h].reshape(2 * ACTS, 384)
    far = theirs[:, f, dyh, h].reshape(2 * ACTS, 384)
    return jnp.where(far_core, far, near)


def chunks_kernel(steps, sc, mine, theirs, *refs):
    blocks, out = refs[:-1], refs[-1]
    for i, (step, block) in enumerate(zip(steps, blocks)):
        a = block[...].reshape(2 * ACTS, 768)
        for f in (0, 1):
            part = dot(chunk_grads(step, f, sc, mine, theirs), a, TT)
            if i == 0:
                out[f] = part
            else:
                out[f] += part


def final_kernel(step, sc, mine, theirs, acc, block, send, keep):
    a = block[...].reshape(2 * ACTS, 768)
    send[...] = (acc[1] + dot(chunk_grads(step, 1, sc, mine, theirs), a, TT)).astype(BF)
    keep[...] = acc[0] + dot(chunk_grads(step, 0, sc, mine, theirs), a, TT)


def sort_kernel(steps, sc, *refs):
    blocks, (tokens, own, send) = refs[: len(steps)], refs[-3:]
    for step, block in zip(steps, blocks):
        src = (sc[Z] - step) & 7
        dc = ((src >> 1) & 1) ^ sc[C]
        for m in range(4):
            peer = sc[YL] ^ m
            tokens[dc, peer, src >> 2, src & 1] = block[m, :NEXT]
            even = block[m, NEXT : NEXT + 24]
            odd = block[m, NEXT + 24 : ROWS]
            own[peer, src] = jnp.where(sc[MY_B] == 1, odd, even)
            send[peer, src] = jnp.where(sc[THEIR_B] == 1, odd, even)


def update_kernel(
    sc, kept, partner, own, got, moment, second, weight, left, tokens,
    update, fresh, away, right, back, half,
):
    right[...] = jnp.where(sc[MY_HAS] == 1, own[...], got[...])
    basis = left[sc[LEFT]]
    gradient = (kept[...] + partner[...].astype(F32)).astype(BF)
    half[...] = dot(basis, gradient, TT).astype(BF)
    for n in range(3):
        cols = slice(256 * n, 256 * n + 256)
        rotated = dot(half[...], right[:, cols], NN)
        new_moment = 0.8 * moment[:, cols] + 0.2 * rotated
        new_second = 0.9 * second[:, cols] + 0.1 * rotated * rotated
        scaled = (new_moment / (jnp.sqrt(new_second) + 1e-08)).astype(BF)
        back[:, cols] = dot(basis, scaled, NN).astype(BF)
    for n in range(3):
        cols = slice(256 * n, 256 * n + 256)
        full = dot(back[...], right[cols, :], NT)
        update[:, cols] = full.astype(BF)
        fresh[:, cols] = (weight[:, cols].astype(F32) - 0.001 * full).astype(BF)
    away[...] = dot(tokens[1], fresh[...], NT).astype(BF)


def keep_kernel(sc, tokens, fresh, keep):
    keep[...] = dot(tokens[0], fresh[...], NT)


def two(near, far, first):
    spots = lax.broadcasted_iota(jnp.int32, (2,) + (1,) * near.ndim, 0)
    return lax.optimization_barrier(jnp.where(spots == first, near[None], far[None]))


def per_device(
    acts, grads, next_acts, weight, moment, second, left_bank, right_bank, left_index, right_index
):
    yl, z, x, yh, c = (lax.axis_index(a) for a in ("yl", "z", "x", "yh", "c"))

    bank_half = lax.dynamic_slice(
        right_bank, (c.astype(jnp.uint32) * 2, jnp.uint32(0), jnp.uint32(0)), (2, 24, 768)
    )
    acts_far = lax.ppermute(acts, "yl", xor(4, 2))
    pairs = []
    for i in range(4):
        for j in range(4):
            there = (i ^ 1) * 4 + (j ^ 1) if (i ^ j) & 1 else i * 4 + j
            if there != i * 4 + j:
                pairs.append((i * 4 + j, there))
    moved = lax.ppermute(grads, ("yl", "x"), pairs)
    grads = lax.optimization_barrier(jnp.where(((yl ^ x) & 1) == 1, moved, grads))
    own = jnp.concatenate([next_acts, bank_half.reshape(BANK, 768)], axis=0)
    others = [lax.ppermute(own, "yl", xor(4, m)) for m in (1, 2, 3)]
    grads_far = lax.ppermute(grads, "yh", ring(2, 1))

    right_own = right_index[0, 0]
    right_far = lax.ppermute(right_index, "c", ring(2, 1))[0, 0]
    values = (
        yl, z, yh, c, left_index[0, 0],
        right_own & 1, ((right_own >> 1) == c).astype(jnp.int32), right_far & 1,
    )
    spots = jnp.arange(len(values), dtype=jnp.int32)
    sc = sum(jnp.where(spots == i, v, 0) for i, v in enumerate(values))

    apart = x ^ yl
    pair = two(grads, grads_far, 0)
    pair_far = lax.ppermute(pair, "x", xor(4, 1))
    quad = two(pair, pair_far, apart & 1)
    quad_far = lax.ppermute(quad, "x", xor(4, 3))
    mine = two(quad, quad_far, apart >> 1)
    theirs = lax.ppermute(mine, "c", ring(2, 1))
    mine = mine.reshape(2, 2, 2, 2, 128, 384)
    theirs = theirs.reshape(2, 2, 2, 2, 128, 384)

    rings = {
        "a": {0: lax.optimization_barrier(jnp.stack([acts, acts_far]))},
        "b": {0: stack_of(own, *others)},
    }
    reach = {"a": (4, 3), "b": (3, 4)}
    for step in (1, 2, 3, 4):
        for k, held in rings.items():
            if step <= reach[k][0]:
                held[step] = lax.ppermute(held[step - 1], "z", ring(8, 1))
            if step <= reach[k][1]:
                held[-step] = lax.ppermute(held[1 - step], "z", ring(8, 7))

    first_steps = (0, 1, -1, 2, -2, 3, -3)
    chunk_flops = 4 * 256 * 384 * 768
    (acc,) = call(
        functools.partial(chunks_kernel, first_steps), [((2, 384, 768), F32)],
        7 * chunk_flops, sc, mine, theirs, *(rings["a"][s] for s in first_steps),
    )
    send, kept = call(
        functools.partial(final_kernel, 4), [((384, 768), BF), ((384, 768), F32)],
        chunk_flops, sc, mine, theirs, acc, rings["a"][4],
    )
    partner = lax.ppermute(send, "yl", xor(4, 1))
    sorted_shapes = [((2, 4, 2, 2, NEXT, 768), BF), ((4, 8, 24, 768), BF), ((4, 8, 24, 768), BF)]
    early = call(
        functools.partial(sort_kernel, first_steps), sorted_shapes, chunk_flops,
        sc, *(rings["b"][s] for s in first_steps),
    )
    tokens, right_mine, right_send = call(
        functools.partial(sort_kernel, (-4,)), sorted_shapes, chunk_flops,
        sc, rings["b"][-4], *early, aliases={2: 0, 3: 1, 4: 2},
    )
    right_got = lax.ppermute(right_send, "c", ring(2, 1))
    tokens = tokens.reshape(2, 512, 768)
    update, fresh, away = pl.pallas_call(
        update_kernel,
        out_shape=[
            jax.ShapeDtypeStruct((384, 768), BF),
            jax.ShapeDtypeStruct((384, 768), BF),
            jax.ShapeDtypeStruct((512, 384), BF),
        ],
        in_specs=[pl.BlockSpec(memory_space=pltpu.SMEM)] + [pl.BlockSpec(memory_space=pltpu.VMEM)] * 9,
        out_specs=[pl.BlockSpec(memory_space=pltpu.VMEM)] * 3,
        scratch_shapes=[
            pltpu.VMEM((768, 768), BF), pltpu.VMEM((384, 768), BF), pltpu.VMEM((384, 768), BF)
        ],
        compiler_params=pltpu.CompilerParams(vmem_limit_bytes=24 * 1024 * 1024),
        cost_estimate=pl.CostEstimate(flops=2 * 10**9, bytes_accessed=10**7, transcendentals=0),
        name="update",
    )(
        sc, kept, partner, right_mine.reshape(768, 768), right_got.reshape(768, 768),
        moment, second, weight, left_bank, tokens,
    )
    away_got = lax.ppermute(away, "c", ring(2, 1))
    (keep,) = call(keep_kernel, [((512, 384), F32)], 3 * 10**8, sc, tokens, fresh)
    keep = (keep + away_got.astype(F32)).astype(BF).reshape(8, 64, 384)
    arrived = lax.all_to_all(keep, ("x", "yh"), split_axis=0, concat_axis=0, tiled=True)
    next_out = arrived.astype(F32).sum(axis=0).astype(BF)
    return update, next_out


def solution(mesh):
    finer = Mesh(mesh.devices.reshape(4, 8, 4, 2, 2), ("yl", "z", "x", "yh", "c"))
    in_specs = (
        P(ROW, COL),
        P(COL, ROW),
        P(ROW, COL),
        P(ROW, COL),
        P(ROW, COL),
        P(ROW, COL),
        P(),
        P(None, ROW, None),
        P(ROW, COL),
        P(ROW, COL),
    )
    out_specs = (P(ROW, COL), P(COL, ROW))

    return jax.shard_map(
        per_device, mesh=finer, in_specs=in_specs, out_specs=out_specs, check_vma=False
    )
```

```python
import functools

import jax
import jax.numpy as jnp
from jax import lax
from jax.experimental import pallas as pl
from jax.experimental.pallas import tpu as pltpu
from jax.sharding import Mesh
from jax.sharding import PartitionSpec as P


ROW = ("yl", "z")
COL = ("x", "yh", "c")
BF = jnp.bfloat16
F32 = jnp.float32


ACTS, NEXT, BANK = 128, 32, 48
ROWS = NEXT + BANK

YL, Z, YH, C, LEFT, MY_B, MY_HAS, THEIR_B = range(8)

TT = (((0,), (0,)), ((), ()))
NT = (((1,), (1,)), ((), ()))
NN = (((1,), (0,)), ((), ()))


def dot(a, b, dims):
    return lax.dot_general(a, b, dims, preferred_element_type=F32)


def stack_of(*parts):
    return lax.optimization_barrier(jnp.stack(parts))


def spread(v):
    for bit in (4, 2):
        v = stack_of(v, lax.ppermute(v, "z", xor(8, bit)))
    return v, lax.ppermute(v, "z", xor(8, 1))


def ring(n, shift):
    return [(i, (i + shift) % n) for i in range(n)]


def xor(n, mask):
    return [(i, i ^ mask) for i in range(n)]


def call(kernel, outs, flops, *args, aliases={}):
    vmem = pl.BlockSpec(memory_space=pltpu.VMEM)
    smem = pl.BlockSpec(memory_space=pltpu.SMEM)
    shapes = [jax.ShapeDtypeStruct(s, d) for s, d in outs]
    nbytes = sum(a.size * a.dtype.itemsize for a in args[1:])
    return pl.pallas_call(
        kernel,
        out_shape=shapes,
        in_specs=[smem] + [vmem] * (len(args) - 1),
        out_specs=[vmem] * len(shapes),
        compiler_params=pltpu.CompilerParams(vmem_limit_bytes=24 * 1024 * 1024),
        cost_estimate=pl.CostEstimate(flops=flops, bytes_accessed=nbytes, transcendentals=0),
        input_output_aliases=aliases,
    )(*args)


SPREAD = [(b, a) for b in (0, 1) for a in (0, 1)]


def source(sc, odd, b, a):
    return sc[Z] ^ (odd + 2 * b + 4 * a)


def chunk_sum(key, f, sc, mine, theirs, block):
    n, odd = key
    parts = []
    for b, a in SPREAD:
        src = source(sc, odd, b, a)
        far_core = (((src >> 1) & 1) ^ sc[C]) == 1
        dyh = (src >> 2) ^ sc[YH]
        h = src & 1
        parts.append(jnp.where(far_core, theirs[f, n, dyh, h], mine[f, n, dyh, h]))
    return dot(jnp.concatenate(parts, axis=0), block[...].reshape(4 * ACTS, 768), TT)


def chunks_kernel(keys, sc, mine, theirs, *refs):
    blocks, out = refs[:-1], refs[-1]
    for i, (key, block) in enumerate(zip(keys, blocks)):
        for f in (0, 1):
            part = chunk_sum(key, f, sc, mine, theirs, block)
            if i == 0:
                out[f] = part
            else:
                out[f] += part


def final_kernel(key, sc, mine, theirs, acc, block, send, keep):
    send[...] = (acc[1] + chunk_sum(key, 1, sc, mine, theirs, block)).astype(BF)
    keep[...] = acc[0] + chunk_sum(key, 0, sc, mine, theirs, block)


def sort_kernel(odd, sc, *refs):
    block, (tokens, own, send) = refs[0], refs[-3:]
    for b, a in SPREAD:
        src = source(sc, odd, b, a)
        dc = ((src >> 1) & 1) ^ sc[C]
        for m in range(4):
            peer = sc[YL] ^ m
            tokens[dc, peer, src >> 2, src & 1] = block[b, a, m, :NEXT]
            first = block[b, a, m, NEXT : NEXT + 24]
            second = block[b, a, m, NEXT + 24 : ROWS]
            own[peer, src] = jnp.where(sc[MY_B] == 1, second, first)
            send[peer, src] = jnp.where(sc[THEIR_B] == 1, second, first)


def update_kernel(
    sc, kept, partner, own, got, moment, second, weight, left, tokens,
    update, fresh, away, right, back, half,
):
    right[...] = jnp.where(sc[MY_HAS] == 1, own[...], got[...])
    basis = left[sc[LEFT]]
    gradient = (kept[...] + partner[...].astype(F32)).astype(BF)
    half[...] = dot(basis, gradient, TT).astype(BF)
    for n in range(3):
        cols = slice(256 * n, 256 * n + 256)
        rotated = dot(half[...], right[:, cols], NN)
        new_moment = 0.8 * moment[:, cols] + 0.2 * rotated
        new_second = 0.9 * second[:, cols] + 0.1 * rotated * rotated
        scaled = (new_moment / (jnp.sqrt(new_second) + 1e-08)).astype(BF)
        back[:, cols] = dot(basis, scaled, NN).astype(BF)
    for n in range(3):
        cols = slice(256 * n, 256 * n + 256)
        full = dot(back[...], right[cols, :], NT)
        update[:, cols] = full.astype(BF)
        fresh[:, cols] = (weight[:, cols].astype(F32) - 0.001 * full).astype(BF)
    away[...] = dot(tokens[1], fresh[...], NT).astype(BF)


def keep_kernel(sc, tokens, fresh, keep):
    keep[...] = dot(tokens[0], fresh[...], NT)


def two(near, far, first):
    spots = lax.broadcasted_iota(jnp.int32, (2,) + (1,) * near.ndim, 0)
    return lax.optimization_barrier(jnp.where(spots == first, near[None], far[None]))


def per_device(
    acts, grads, next_acts, weight, moment, second, left_bank, right_bank, left_index, right_index
):
    yl, z, x, yh, c = (lax.axis_index(a) for a in ("yl", "z", "x", "yh", "c"))

    bank_half = lax.dynamic_slice(
        right_bank, (c.astype(jnp.uint32) * 2, jnp.uint32(0), jnp.uint32(0)), (2, 24, 768)
    )
    acts_far = lax.ppermute(acts, "yl", xor(4, 2))
    pairs = []
    for i in range(4):
        for j in range(4):
            there = (i ^ 1) * 4 + (j ^ 1) if (i ^ j) & 1 else i * 4 + j
            if there != i * 4 + j:
                pairs.append((i * 4 + j, there))
    moved = lax.ppermute(grads, ("yl", "x"), pairs)
    grads = lax.optimization_barrier(jnp.where(((yl ^ x) & 1) == 1, moved, grads))
    own = jnp.concatenate([next_acts, bank_half.reshape(BANK, 768)], axis=0)
    others = [lax.ppermute(own, "yl", xor(4, m)) for m in (1, 2, 3)]
    grads_far = lax.ppermute(grads, "yh", ring(2, 1))

    right_own = right_index[0, 0]
    right_far = lax.ppermute(right_index, "c", ring(2, 1))[0, 0]
    values = (
        yl, z, yh, c, left_index[0, 0],
        right_own & 1, ((right_own >> 1) == c).astype(jnp.int32), right_far & 1,
    )
    spots = jnp.arange(len(values), dtype=jnp.int32)
    sc = sum(jnp.where(spots == i, v, 0) for i, v in enumerate(values))

    apart = x ^ yl
    pair = two(grads, grads_far, 0)
    pair_far = lax.ppermute(pair, "x", xor(4, 2))
    quad = two(pair, pair_far, apart >> 1)
    quad_far = lax.ppermute(quad, "x", xor(4, 1))
    mine = two(quad, quad_far, apart & 1)
    theirs = lax.ppermute(mine, "c", ring(2, 1))
    mine = mine.reshape(2, 2, 2, 2, 128, 384)
    theirs = theirs.reshape(2, 2, 2, 2, 128, 384)

    near, far = spread(acts), spread(acts_far)
    rest = spread(stack_of(own, *others))

    chunk_flops = 4 * 512 * 384 * 768
    (acc,) = call(
        functools.partial(chunks_kernel, ((0, 0), (0, 1), (1, 0))), [((2, 384, 768), F32)],
        3 * chunk_flops, sc, mine, theirs, *near, far[0],
    )
    send, kept = call(
        functools.partial(final_kernel, (1, 1)), [((384, 768), BF), ((384, 768), F32)],
        chunk_flops, sc, mine, theirs, acc, far[1],
    )
    partner = lax.ppermute(send, "yl", xor(4, 1))
    sorted_shapes = [((2, 4, 2, 2, NEXT, 768), BF), ((4, 8, 24, 768), BF), ((4, 8, 24, 768), BF)]
    early = call(functools.partial(sort_kernel, 0), sorted_shapes, chunk_flops, sc, rest[0])
    tokens, right_mine, right_send = call(
        functools.partial(sort_kernel, 1), sorted_shapes, chunk_flops,
        sc, rest[1], *early, aliases={2: 0, 3: 1, 4: 2},
    )
    right_got = lax.ppermute(right_send, "c", ring(2, 1))
    tokens = tokens.reshape(2, 512, 768)
    update, fresh, away = pl.pallas_call(
        update_kernel,
        out_shape=[
            jax.ShapeDtypeStruct((384, 768), BF),
            jax.ShapeDtypeStruct((384, 768), BF),
            jax.ShapeDtypeStruct((512, 384), BF),
        ],
        in_specs=[pl.BlockSpec(memory_space=pltpu.SMEM)] + [pl.BlockSpec(memory_space=pltpu.VMEM)] * 9,
        out_specs=[pl.BlockSpec(memory_space=pltpu.VMEM)] * 3,
        scratch_shapes=[
            pltpu.VMEM((768, 768), BF), pltpu.VMEM((384, 768), BF), pltpu.VMEM((384, 768), BF)
        ],
        compiler_params=pltpu.CompilerParams(vmem_limit_bytes=24 * 1024 * 1024),
        cost_estimate=pl.CostEstimate(flops=2 * 10**9, bytes_accessed=10**7, transcendentals=0),
        name="update",
    )(
        sc, kept, partner, right_mine.reshape(768, 768), right_got.reshape(768, 768),
        moment, second, weight, left_bank, tokens,
    )
    away_got = lax.ppermute(away, "c", ring(2, 1))
    (keep,) = call(keep_kernel, [((512, 384), F32)], 3 * 10**8, sc, tokens, fresh)
    keep = (keep + away_got.astype(F32)).astype(BF).reshape(8, 64, 384)
    arrived = lax.all_to_all(keep, ("x", "yh"), split_axis=0, concat_axis=0, tiled=True)
    next_out = arrived.astype(F32).sum(axis=0).astype(BF)
    return update, next_out


def solution(mesh):
    finer = Mesh(mesh.devices.reshape(4, 8, 4, 2, 2), ("yl", "z", "x", "yh", "c"))
    in_specs = (
        P(ROW, COL),
        P(COL, ROW),
        P(ROW, COL),
        P(ROW, COL),
        P(ROW, COL),
        P(ROW, COL),
        P(),
        P(None, ROW, None),
        P(ROW, COL),
        P(ROW, COL),
    )
    out_specs = (P(ROW, COL), P(COL, ROW))

    return jax.shard_map(
        per_device, mesh=finer, in_specs=in_specs, out_specs=out_specs, check_vma=False
    )
```

```python
import functools

import jax
import jax.numpy as jnp
from jax import lax
from jax.experimental import pallas as pl
from jax.experimental.pallas import tpu as pltpu
from jax.sharding import Mesh
from jax.sharding import PartitionSpec as P


ROW = ("yl", "z")
COL = ("x", "yh", "c")
BF = jnp.bfloat16
F32 = jnp.float32


ACTS, NEXT, BANK = 128, 32, 48
ROWS = NEXT + BANK

YL, Z, YH, C, LEFT, MY_B, MY_HAS, THEIR_B = range(8)

TT = (((0,), (0,)), ((), ()))
NT = (((1,), (1,)), ((), ()))
NN = (((1,), (0,)), ((), ()))


def dot(a, b, dims):
    return lax.dot_general(a, b, dims, preferred_element_type=F32)


def stack_of(*parts):
    return lax.optimization_barrier(jnp.stack(parts))


def ring(n, shift):
    return [(i, (i + shift) % n) for i in range(n)]


def xor(n, mask):
    return [(i, i ^ mask) for i in range(n)]


def call(kernel, outs, flops, *args, aliases={}):
    vmem = pl.BlockSpec(memory_space=pltpu.VMEM)
    smem = pl.BlockSpec(memory_space=pltpu.SMEM)
    shapes = [jax.ShapeDtypeStruct(s, d) for s, d in outs]
    nbytes = sum(a.size * a.dtype.itemsize for a in args[1:])
    return pl.pallas_call(
        kernel,
        out_shape=shapes,
        in_specs=[smem] + [vmem] * (len(args) - 1),
        out_specs=[vmem] * len(shapes),
        compiler_params=pltpu.CompilerParams(vmem_limit_bytes=24 * 1024 * 1024),
        cost_estimate=pl.CostEstimate(flops=flops, bytes_accessed=nbytes, transcendentals=0),
        input_output_aliases=aliases,
    )(*args)


def chunk_grads(step, f, sc, mine, theirs):
    src = (sc[Z] - step) & 7
    far_core = (((src >> 1) & 1) ^ sc[C]) == 1
    dyh = (src >> 2) ^ sc[YH]
    h = src & 1
    near = mine[:, f, dyh, h].reshape(2 * ACTS, 384)
    far = theirs[:, f, dyh, h].reshape(2 * ACTS, 384)
    return jnp.where(far_core, far, near)


def chunks_kernel(steps, sc, mine, theirs, *refs):
    blocks, out = refs[:-1], refs[-1]
    for i, (step, block) in enumerate(zip(steps, blocks)):
        a = block[...].reshape(2 * ACTS, 768)
        for f in (0, 1):
            part = dot(chunk_grads(step, f, sc, mine, theirs), a, TT)
            if i == 0:
                out[f] = part
            else:
                out[f] += part


def final_kernel(step, f, sc, mine, theirs, acc, block, out):
    a = block[...].reshape(2 * ACTS, 768)
    out[...] = (acc[f] + dot(chunk_grads(step, f, sc, mine, theirs), a, TT)).astype(out.dtype)


def sort_kernel(steps, sc, *refs):
    blocks, (tokens, own, send) = refs[: len(steps)], refs[-3:]
    for step, block in zip(steps, blocks):
        src = (sc[Z] - step) & 7
        dc = ((src >> 1) & 1) ^ sc[C]
        for m in range(4):
            peer = sc[YL] ^ m
            tokens[dc, peer, src >> 2, src & 1] = block[m, :NEXT]
            even = block[m, NEXT : NEXT + 24]
            odd = block[m, NEXT + 24 : ROWS]
            own[peer, src] = jnp.where(sc[MY_B] == 1, odd, even)
            send[peer, src] = jnp.where(sc[THEIR_B] == 1, odd, even)


def update_kernel(
    sc, kept, partner, own, got, moment, second, weight, left, tokens,
    update, fresh, away, right, back, half,
):
    right[...] = jnp.where(sc[MY_HAS] == 1, own[...], got[...])
    basis = left[sc[LEFT]]
    gradient = (kept[...] + partner[...].astype(F32)).astype(BF)
    half[...] = dot(basis, gradient, TT).astype(BF)
    for n in range(3):
        cols = slice(256 * n, 256 * n + 256)
        rotated = dot(half[...], right[:, cols], NN)
        new_moment = 0.8 * moment[:, cols] + 0.2 * rotated
        new_second = 0.9 * second[:, cols] + 0.1 * rotated * rotated
        scaled = (new_moment / (jnp.sqrt(new_second) + 1e-08)).astype(BF)
        back[:, cols] = dot(basis, scaled, NN).astype(BF)
    for n in range(3):
        cols = slice(256 * n, 256 * n + 256)
        full = dot(back[...], right[cols, :], NT)
        update[:, cols] = full.astype(BF)
        fresh[:, cols] = (weight[:, cols].astype(F32) - 0.001 * full).astype(BF)
    away[...] = dot(tokens[1], fresh[...], NT).astype(BF)


def keep_kernel(sc, tokens, fresh, keep):
    keep[...] = dot(tokens[0], fresh[...], NT)


def two(near, far, first):
    spots = lax.broadcasted_iota(jnp.int32, (2,) + (1,) * near.ndim, 0)
    return lax.optimization_barrier(jnp.where(spots == first, near[None], far[None]))


def per_device(
    acts, grads, next_acts, weight, moment, second, left_bank, right_bank, left_index, right_index
):
    yl, z, x, yh, c = (lax.axis_index(a) for a in ("yl", "z", "x", "yh", "c"))

    bank_half = lax.dynamic_slice(
        right_bank, (c.astype(jnp.uint32) * 2, jnp.uint32(0), jnp.uint32(0)), (2, 24, 768)
    )
    acts_far = lax.ppermute(acts, "yl", xor(4, 2))
    pairs = []
    for i in range(4):
        for j in range(4):
            there = (i ^ 1) * 4 + (j ^ 1) if (i ^ j) & 1 else i * 4 + j
            if there != i * 4 + j:
                pairs.append((i * 4 + j, there))
    moved = lax.ppermute(grads, ("yl", "x"), pairs)
    grads = lax.optimization_barrier(jnp.where(((yl ^ x) & 1) == 1, moved, grads))
    own = jnp.concatenate([next_acts, bank_half.reshape(BANK, 768)], axis=0)
    others = [lax.ppermute(own, "yl", xor(4, m)) for m in (1, 2, 3)]
    grads_far = lax.ppermute(grads, "yh", ring(2, 1))

    right_own = right_index[0, 0]
    right_far = lax.ppermute(right_index, "c", ring(2, 1))[0, 0]
    values = (
        yl, z, yh, c, left_index[0, 0],
        right_own & 1, ((right_own >> 1) == c).astype(jnp.int32), right_far & 1,
    )
    spots = jnp.arange(len(values), dtype=jnp.int32)
    sc = sum(jnp.where(spots == i, v, 0) for i, v in enumerate(values))

    apart = x ^ yl
    pair = two(grads, grads_far, 0)
    pair_far = lax.ppermute(pair, "x", xor(4, 1))
    quad = two(pair, pair_far, apart & 1)
    quad_far = lax.ppermute(quad, "x", xor(4, 3))
    mine = two(quad, quad_far, apart >> 1)
    theirs = lax.ppermute(mine, "c", ring(2, 1))
    mine = mine.reshape(2, 2, 2, 2, 128, 384)
    theirs = theirs.reshape(2, 2, 2, 2, 128, 384)

    rings = {
        "a": {0: lax.optimization_barrier(jnp.stack([acts, acts_far]))},
        "b": {0: stack_of(own, *others)},
    }
    reach = {"a": (4, 3), "b": (3, 4)}
    for step in (1, 2, 3, 4):
        for k, held in rings.items():
            if step <= reach[k][0]:
                held[step] = lax.ppermute(held[step - 1], "z", ring(8, 1))
            if step <= reach[k][1]:
                held[-step] = lax.ppermute(held[1 - step], "z", ring(8, 7))

    first_steps = (0, 1, -1, 2, -2, 3, -3)
    chunk_flops = 4 * 256 * 384 * 768
    (acc,) = call(
        functools.partial(chunks_kernel, first_steps), [((2, 384, 768), F32)],
        7 * chunk_flops, sc, mine, theirs, *(rings["a"][s] for s in first_steps),
    )
    (send,) = call(
        functools.partial(final_kernel, 4, 1), [((384, 768), BF)],
        chunk_flops // 2, sc, mine, theirs, acc, rings["a"][4],
    )
    partner = lax.ppermute(send, "yl", xor(4, 1))
    (kept,) = call(
        functools.partial(final_kernel, 4, 0), [((384, 768), F32)],
        chunk_flops // 2, sc, mine, theirs, acc, rings["a"][4],
    )
    sorted_shapes = [((2, 4, 2, 2, NEXT, 768), BF), ((4, 8, 24, 768), BF), ((4, 8, 24, 768), BF)]
    early = call(
        functools.partial(sort_kernel, first_steps), sorted_shapes, chunk_flops,
        sc, *(rings["b"][s] for s in first_steps),
    )
    tokens, right_mine, right_send = call(
        functools.partial(sort_kernel, (-4,)), sorted_shapes, chunk_flops,
        sc, rings["b"][-4], *early, aliases={2: 0, 3: 1, 4: 2},
    )
    right_got = lax.ppermute(right_send, "c", ring(2, 1))
    tokens = tokens.reshape(2, 512, 768)
    update, fresh, away = pl.pallas_call(
        update_kernel,
        out_shape=[
            jax.ShapeDtypeStruct((384, 768), BF),
            jax.ShapeDtypeStruct((384, 768), BF),
            jax.ShapeDtypeStruct((512, 384), BF),
        ],
        in_specs=[pl.BlockSpec(memory_space=pltpu.SMEM)] + [pl.BlockSpec(memory_space=pltpu.VMEM)] * 9,
        out_specs=[pl.BlockSpec(memory_space=pltpu.VMEM)] * 3,
        scratch_shapes=[
            pltpu.VMEM((768, 768), BF), pltpu.VMEM((384, 768), BF), pltpu.VMEM((384, 768), BF)
        ],
        compiler_params=pltpu.CompilerParams(vmem_limit_bytes=24 * 1024 * 1024),
        cost_estimate=pl.CostEstimate(flops=2 * 10**9, bytes_accessed=10**7, transcendentals=0),
        name="update",
    )(
        sc, kept, partner, right_mine.reshape(768, 768), right_got.reshape(768, 768),
        moment, second, weight, left_bank, tokens,
    )
    away_got = lax.ppermute(away, "c", ring(2, 1))
    (keep,) = call(keep_kernel, [((512, 384), F32)], 3 * 10**8, sc, tokens, fresh)
    keep = (keep + away_got.astype(F32)).astype(BF).reshape(8, 64, 384)
    arrived = lax.all_to_all(keep, ("x", "yh"), split_axis=0, concat_axis=0, tiled=True)
    next_out = arrived.astype(F32).sum(axis=0).astype(BF)
    return update, next_out


def solution(mesh):
    finer = Mesh(mesh.devices.reshape(4, 8, 4, 2, 2), ("yl", "z", "x", "yh", "c"))
    in_specs = (
        P(ROW, COL),
        P(COL, ROW),
        P(ROW, COL),
        P(ROW, COL),
        P(ROW, COL),
        P(ROW, COL),
        P(),
        P(None, ROW, None),
        P(ROW, COL),
        P(ROW, COL),
    )
    out_specs = (P(ROW, COL), P(COL, ROW))

    return jax.shard_map(
        per_device, mesh=finer, in_specs=in_specs, out_specs=out_specs, check_vma=False
    )
```
